32 devices in a mesh: rows: 8 (over z, y), cols: 4 (over x, core).
Axes of the slice: x: 2, y: 2, z: 4, core: 2. Of those that a mesh axis runs over, the one named last changes fastest.
Arguments:
- gradients: float32 [32, 128, 4096], P(None, 'rows', 'cols'), may hold values from -6 to 6
- momentum: float32 [32, 128, 4096], P(None, 'rows', 'cols'), may hold values from -6 to 6
- weights: float32 [32, 128, 4096], P(None, 'rows', 'cols'), may hold values from -0.1875 to 0.1875
Outputs:
- new_weights: float32 [32, 128, 4096], P(None, 'rows', 'cols')
- new_momentum: float32 [32, 128, 4096], P(None, 'rows', 'cols')
The draws below stay inside these ranges and needn't reach their ends.
All inputs are finite; a program needn't handle non-finite values.
Results may differ from the reference program's by a relative error of at most 0.0003.
Values sent between devices are 32-bit elements.
A program may use at most 64 MiB of HBM per device.

```python
import jax
import jax.numpy as jnp
from jax import lax

SIDE = 128
WIDE = 4096
MATS = 32
ITERS = 4


def level_of(stream_key, dims, pieces, least, largest):
    def one(dim, blocks):
        steps = jax.random.uniform(jax.random.fold_in(jax.random.fold_in(stream_key, 6), dim), (blocks,), jnp.float32, least / len(pieces), largest / len(pieces))
        return jnp.repeat(jnp.exp(steps), dims[dim] // blocks).reshape((-1,) + (1,) * (len(dims) - dim - 1))

    gain = one(*pieces[0])
    for cut in pieces[1:]:
        gain = gain * one(*cut)
    return gain


def noise(stream_key, extent, scale, limit, cuts=(), kind=jnp.bfloat16):
    result = scale * jax.random.normal(stream_key, extent, jnp.float32)
    if cuts:
        result = result * level_of(stream_key, extent, cuts, -0.22, 0.18)
    return jnp.clip(result, -limit, limit).astype(kind)


def setup_inputs(seed: int = 0) -> dict:
    streams_of = jax.random.split(jax.random.key(seed), 4)
    return {
        "gradients": noise(streams_of[0], (MATS, SIDE, WIDE), 1.0, 6.0, ((1, 8), (2, 4)), jnp.float32),
        "momentum": noise(streams_of[1], (MATS, SIDE, WIDE), 1.0, 6.0, ((1, 8), (2, 4)), jnp.float32),
        "weights": noise(streams_of[2], (MATS, SIDE, WIDE), 0.03, 0.1875, ((1, 8), (2, 4)), jnp.float32),
    }


hold_rate = 0.8
learn_rate = 0.8
decay_rate = 0.1

def reference(gradients, momentum, weights):
    new_momentum = hold_rate * momentum + gradients

    def orthogonal_one(stack):
        iterate = stack[None]
        iterate = iterate * lax.rsqrt(lax.optimization_barrier(jnp.sum(iterate * iterate, axis=(1, 2), keepdims=True)) + 1e-06)
        for step in range(ITERS):
            gram = jnp.einsum('mik,mjk->mij', iterate, iterate, precision=lax.Precision.HIGHEST)
            mixed = -4.775 * gram + 2.0315 * jnp.einsum('mij,mjk->mik', gram, gram, precision=lax.Precision.HIGHEST)
            iterate = 3.4445 * iterate + jnp.einsum('mij,mjk->mik', mixed, iterate, precision=lax.Precision.HIGHEST)
        return iterate[0]
    iterate = lax.map(orthogonal_one, new_momentum)
    new_weights = (1.0 - learn_rate * decay_rate) * weights - learn_rate * iterate
    return (new_weights, new_momentum)
```

```python
import jax
import jax.numpy as jnp
from jax import lax
from jax.sharding import PartitionSpec as P

ITERS = 4


hold_rate = 0.8
learn_rate = 0.8
decay_rate = 0.1


def mul(a, b):
    return jnp.einsum("mij,mjk->mik", a, b, precision=lax.Precision.HIGHEST)


def local(gradients, momentum, weights):
    new_momentum = hold_rate * momentum + gradients
    whole = lax.all_to_all(new_momentum, "rows", split_axis=0, concat_axis=1, tiled=True)
    gram = jnp.einsum("mik,mjk->mij", whole, whole, precision=lax.Precision.HIGHEST)
    gram = lax.psum(gram, "cols")
    eye = jnp.eye(gram.shape[-1], dtype=jnp.float32)
    total = jnp.sum(gram * eye, axis=(1, 2), keepdims=True)
    scale = lax.rsqrt(total + 1e-06)
    gram = gram * scale * scale
    chain = scale * eye
    for step in range(ITERS):
        factor = 3.4445 * eye - 4.775 * gram + 2.0315 * mul(gram, gram)
        chain = mul(factor, chain)
        if step < ITERS - 1:
            gram = mul(factor, mul(gram, factor))
    iterate = mul(chain, whole)
    back = lax.all_to_all(iterate, "rows", split_axis=1, concat_axis=0, tiled=True)
    new_weights = (1.0 - learn_rate * decay_rate) * weights - learn_rate * back
    return (new_weights, new_momentum)


def solution(mesh):
    placed = (P(None, "rows", "cols"), P(None, "rows", "cols"), P(None, "rows", "cols"))
    return jax.shard_map(
        local,
        mesh=mesh,
        in_specs=placed,
        out_specs=(P(None, "rows", "cols"), P(None, "rows", "cols")),
        check_vma=False,
    )
```

```python
import functools

import jax
import jax.numpy as jnp
from jax import lax
from jax.experimental import pallas as pl
from jax.experimental.pallas import tpu as pltpu
from jax.sharding import PartitionSpec as P

ITERS = 4


hold_rate = 0.8
learn_rate = 0.8
decay_rate = 0.1

MESH = pl.DeviceIdType.MESH


def split(x):
    high = x.astype(jnp.bfloat16)
    return high, (x - high.astype(jnp.float32)).astype(jnp.bfloat16)


def dot(a, b):
    return jnp.dot(a, b, preferred_element_type=jnp.float32)


def mul(a, b):
    side = b.shape[1]
    ah, al = split(a)
    bh, bl = split(b)
    right = jnp.concatenate([bh, bl], axis=1)
    out = dot(jnp.concatenate([ah, al], axis=1), jnp.concatenate([right, right], axis=0))
    return out[:, :side] + out[:, side:]


def gram_of(block, side, wide, tile):
    total = None
    for at in range(0, wide, tile):
        high, low = split(block[:, :, at : at + tile].reshape(side, tile))
        both = jnp.concatenate([high, low], axis=0)
        part = lax.dot_general(high, both, (((1,), (1,)), ((), ())), preferred_element_type=jnp.float32)
        total = part if total is None else total + part
    cross = total[:, side:]
    return total[:, :side] + cross + cross.T


def chain_of(gram):
    side = gram.shape[0]
    eye = (
        lax.broadcasted_iota(jnp.int32, (side, side), 0) == lax.broadcasted_iota(jnp.int32, (side, side), 1)
    ).astype(jnp.float32)
    total = jnp.sum(gram * eye, axis=(0, 1), keepdims=True)
    scale = lax.rsqrt(total + 1e-06)
    gram = gram * scale * scale
    chain = None
    for step in range(ITERS):
        factor = 3.4445 * eye - 4.775 * gram + 2.0315 * mul(gram, gram)
        chain = factor if chain is None else mul(factor, chain)
        if step < ITERS - 1:
            gram = mul(factor, mul(gram, factor))
    return chain * scale


def kernel(n, c, nm_ref, w_ref, out_ref, seen, grams, sent, back, w_buf,
           load_sem, own_sem, s1, r1, sg, rg, s2, r2, out_sem):
    _, per, b, wide = nm_ref.shape
    side = n * b
    me, my = lax.axis_index("rows"), lax.axis_index("cols")

    own = [pltpu.make_async_copy(nm_ref.at[me, j], seen.at[j, me], own_sem.at[j]) for j in range(per)]
    for copy in own:
        copy.start()
    load = pltpu.make_async_copy(w_ref, w_buf, load_sem)
    load.start()

    barrier = pltpu.get_barrier_semaphore()
    for k in range(1, n):
        pl.semaphore_signal(barrier, inc=1, device_id={"rows": lax.rem(me + k, n)}, device_id_type=MESH)
    for k in range(1, c):
        pl.semaphore_signal(barrier, inc=1, device_id={"cols": lax.rem(my + k, c)}, device_id_type=MESH)
    pl.semaphore_wait(barrier, n - 1 + c - 1)

    def there(j, k):
        to = lax.rem(me + k, n)
        return pltpu.make_async_remote_copy(
            src_ref=nm_ref.at[to, j], dst_ref=seen.at[j, me],
            send_sem=s1.at[j, k], recv_sem=r1.at[j, k],
            device_id={"rows": to}, device_id_type=MESH)

    def home(j, k):
        to = lax.rem(me + k, n)
        return pltpu.make_async_remote_copy(
            src_ref=sent.at[j, to], dst_ref=back.at[j, me],
            send_sem=s2.at[j, k], recv_sem=r2.at[j, k],
            device_id={"rows": to}, device_id_type=MESH)

    def across(j, k):
        return pltpu.make_async_remote_copy(
            src_ref=grams.at[j, my], dst_ref=grams.at[j, my],
            send_sem=sg.at[j, k], recv_sem=rg.at[j, k],
            device_id={"cols": lax.rem(my + k, c)}, device_id_type=MESH)

    for j in range(per):
        for k in range(1, n):
            there(j, k).start()

    tile = min(256, wide)

    def gram(j):
        own[j].wait()
        for k in range(1, n):
            there(j, k).wait_recv()
        grams[j, my] = gram_of(seen[j], side, wide, tile)
        for k in range(1, c):
            across(j, k).start()

    def step(j):
        for k in range(1, c):
            across(j, k).wait_recv()
        total = grams[j, 0]
        for k in range(1, c):
            total = total + grams[j, k]
        high, low = split(chain_of(total))
        left = jnp.concatenate([high, low], axis=1)
        for at in range(0, wide, tile):
            xh, xl = split(seen[j, :, :, at : at + tile].reshape(side, tile))
            part = dot(left, jnp.concatenate([xh, xh], axis=0)) + dot(high, xl)
            sent[j, :, :, at : at + tile] = part.reshape(n, b, tile)
        for k in range(1, n):
            home(j, k).start()
        back[j, me] = sent[j, me]

    def finish(j):
        for k in range(1, n):
            home(j, k).wait_recv()
        w_buf[:, j] = (1.0 - learn_rate * decay_rate) * w_buf[:, j] - learn_rate * back[j]
        pltpu.make_async_copy(w_buf.at[:, j], out_ref.at[:, j], out_sem.at[j]).start()

    gram(0)
    for j in range(per):
        if j + 1 < per:
            gram(j + 1)
        step(j)
    load.wait()
    for j in range(per):
        finish(j)
    for j in range(per):
        for k in range(1, n):
            there(j, k).wait_send()
            home(j, k).wait_send()
        for k in range(1, c):
            across(j, k).wait_send()
        pltpu.make_async_copy(w_buf.at[:, j], out_ref.at[:, j], out_sem.at[j]).wait()


def exchange_in_kernel(n, c, new_momentum, weights):
    mats, b, wide = weights.shape
    per, side = mats // n, n * b
    shape = (n, per, b, wide)
    dma = pltpu.SemaphoreType.DMA
    f32 = jnp.float32
    out = pl.pallas_call(
        functools.partial(kernel, n, c),
        out_shape=jax.ShapeDtypeStruct(shape, f32),
        in_specs=[pl.BlockSpec(memory_space=pl.ANY)] * 2,
        out_specs=pl.BlockSpec(memory_space=pl.ANY),
        scratch_shapes=[
            pltpu.VMEM((per, n, b, wide), f32),
            pltpu.VMEM((per, c, side, side), f32),
            pltpu.VMEM((per, n, b, wide), f32),
            pltpu.VMEM((per, n, b, wide), f32),
            pltpu.VMEM((n, per, b, wide), f32),
            dma, dma((per,)),
            dma((per, n)), dma((per, n)),
            dma((per, c)), dma((per, c)),
            dma((per, n)), dma((per, n)),
            dma((per,)),
        ],
        compiler_params=pltpu.CompilerParams(
            collective_id=0, has_side_effects=True, vmem_limit_bytes=40 * 2**20
        ),
    )(new_momentum.reshape(shape), weights.reshape(shape))
    return out.reshape(weights.shape)


def product(a, b):
    return jnp.einsum("mij,mjk->mik", a, b, precision=lax.Precision.HIGHEST)


def exchange_in_xla(new_momentum, weights):
    whole = lax.all_to_all(new_momentum, "rows", split_axis=0, concat_axis=1, tiled=True)
    gram = jnp.einsum("mik,mjk->mij", whole, whole, precision=lax.Precision.HIGHEST)
    gram = lax.psum(gram, "cols")
    eye = jnp.eye(gram.shape[-1], dtype=jnp.float32)
    total = jnp.sum(gram * eye, axis=(1, 2), keepdims=True)
    scale = lax.rsqrt(total + 1e-06)
    gram = gram * scale * scale
    chain = scale * eye
    for step in range(ITERS):
        factor = 3.4445 * eye - 4.775 * gram + 2.0315 * product(gram, gram)
        chain = product(factor, chain)
        if step < ITERS - 1:
            gram = product(factor, product(gram, factor))
    iterate = product(chain, whole)
    back = lax.all_to_all(iterate, "rows", split_axis=1, concat_axis=0, tiled=True)
    return (1.0 - learn_rate * decay_rate) * weights - learn_rate * back


def local(n, c, gradients, momentum, weights):
    new_momentum = hold_rate * momentum + gradients
    if weights.shape[1] % 8 == 0:
        new_weights = exchange_in_kernel(n, c, new_momentum, weights)
    else:
        new_weights = exchange_in_xla(new_momentum, weights)
    return (new_weights, new_momentum)


def solution(mesh):
    placed = (P(None, "rows", "cols"), P(None, "rows", "cols"), P(None, "rows", "cols"))
    return jax.shard_map(
        functools.partial(local, mesh.shape["rows"], mesh.shape["cols"]),
        mesh=mesh,
        in_specs=placed,
        out_specs=(P(None, "rows", "cols"), P(None, "rows", "cols")),
        check_vma=False,
    )
```
